32 devices in a mesh: groups: 2 (over x), blk: 16 (over z, y, core).
Axes of the slice: x: 2, y: 2, z: 4, core: 2. Of those that a mesh axis runs over, the one named last changes fastest.
Arguments:
- walkers: bfloat16 [64, 65536], P(('groups', 'blk')), parts along dimension 0, may hold values from -6 to 6
- intersection_inv: bfloat16 [64, 4096], P(('groups', 'blk')), parts along dimension 0, may hold values from -0.75 to 0.75
- new_slot: int32 [64], P(('groups', 'blk')), parts along dimension 0, may hold values from 0 to 31, as said below
- cholesky: bfloat16 [2048, 64, 10240], P(('groups', 'blk')), parts along dimension 0, may hold values from -0.0234375 to 0.0234375
Outputs:
- moved_walkers: bfloat16 [64, 65536], P(('groups', 'blk')), parts along dimension 0
- moved_intersection_inv: bfloat16 [64, 4096], P(('groups', 'blk')), parts along dimension 0
- force_bias: float32 [64, 10240], P(('groups', 'blk')), parts along dimension 0
The draws below stay inside these ranges and needn't reach their ends.
There are 2 independent parts, one for each index of `groups`. The reference program is written for one: setup_inputs(seed, part) draws one part's arguments, and reference() takes and returns one part's arrays. A program takes and returns all parts, laid end to end along the dimension named above; each array names one. Nothing has to cross between parts.
Inputs may be any that keep to these rules, and one draw needn't show every extreme that they name: new_slot is a permutation; the new owner of walker w is new_slot[w] // 2; the 2 walkers of one device go to 2 different owners, and new_slot[w] % 2 == w % 2.
All inputs are finite; a program needn't handle non-finite values.
Results may differ from the reference program's by a relative error of at most 0.0028.
Values may be sent and summed in bfloat16 or wider, within the bound.
No kernel may reach another device: no remote copies, remote signals or barrier semaphores. Data moves between devices by JAX's collectives and lax.ppermute only.
A program may use at most 128 MiB of HBM per device.

```python
import jax
import jax.numpy as jnp
from jax import lax

M = 1024
NOCC = 64
NCHOL = 10240
W_DEV = 2
W_TOTAL = 32
N_BLK = 16


def draw_new_slot(key, part):
    device_count = W_TOTAL // W_DEV
    key_one, key_two = jax.random.split(jax.random.fold_in(key, 17))
    rotation = jax.random.permutation(key_one, device_count)
    relabel = jax.random.permutation(key_two, device_count)
    device_ids = jnp.arange(W_TOTAL, dtype=jnp.int32) // W_DEV
    local_ids = jnp.arange(W_TOTAL, dtype=jnp.int32) % W_DEV
    owners = relabel[(rotation[device_ids] + local_ids) % device_count]
    return (owners * W_DEV + local_ids).astype(jnp.int32)


def steps_of(rng, dims, pieces, least, high):
    def one(position, parts):
        heights = jax.random.uniform(jax.random.fold_in(jax.random.fold_in(rng, 6), position), (parts,), jnp.float32, least / len(pieces), high / len(pieces))
        return jnp.repeat(jnp.exp(heights), dims[position] // parts).reshape((-1,) + (1,) * (len(dims) - position - 1))

    gain = one(*pieces[0])
    for cut in pieces[1:]:
        gain = gain * one(*cut)
    return gain


def noise(key, dims, scale, most, cuts=(), kind=jnp.bfloat16):
    drawn = jax.random.normal(key, dims, jnp.float32) * scale
    if len(cuts) > 0:
        drawn = steps_of(key, dims, cuts, -0.22, 0.18) * drawn
    return jnp.clip(drawn, min=-most, max=most).astype(kind)


def setup_inputs(seed: int = 0, part: int = 0) -> dict:
    keys = jax.random.split(jax.random.key(seed), 5)
    own_keys = jax.random.split(jax.random.fold_in(keys[4], part), 5)
    return {
        "walkers": noise(own_keys[0], (W_TOTAL, M * NOCC), 1.0, 6.0, ((0, 16),)),
        "intersection_inv": noise(own_keys[1], (W_TOTAL, NOCC * NOCC), NOCC ** -0.5, 0.75, ((0, 16),)),
        "new_slot": draw_new_slot(jax.random.fold_in(jax.random.fold_in(keys[4], part), 71), part),
        "cholesky": noise(own_keys[3], (M, NOCC, NCHOL), (M * NOCC) ** -0.5, 0.0234375, ((0, 16),)),
    }


def reference(walkers, intersection_inv, new_slot, cholesky):
    walker_total = walkers.shape[0]
    anchor = jnp.zeros((walker_total,), jnp.int32).at[new_slot].set(jnp.arange(walker_total, dtype=jnp.int32))
    moved_walkers = walkers[anchor]
    moved_inverse = intersection_inv[anchor]
    greens = jnp.einsum('wpj,wij->wpi', moved_walkers.reshape(walker_total, M, NOCC).astype(jnp.float32), moved_inverse.reshape(walker_total, NOCC, NOCC).astype(jnp.float32)).astype(jnp.bfloat16)
    blocks = greens.reshape(walker_total, N_BLK, (M // N_BLK) * NOCC).transpose(1, 0, 2)
    chol_blocks = cholesky.reshape(N_BLK, (M // N_BLK) * NOCC, NCHOL)

    def add_block(running, operands):
        return running + jnp.dot(operands[0], operands[1], preferred_element_type=jnp.float32), None

    force_bias, _ = lax.scan(add_block, jnp.zeros((walker_total, NCHOL), jnp.float32), (blocks, chol_blocks))
    return moved_walkers, moved_inverse, force_bias
```

```python
import jax
import jax.numpy as jnp
from jax import lax
from jax.experimental import pallas as pl
from jax.experimental.pallas import tpu as pltpu
from jax.sharding import PartitionSpec as P


BF = jnp.bfloat16
F32 = jnp.float32
LANES = 128
SLOT_ROWS = 4
RADIX = 256


def greens_kernel(slot_ref, walk_ref, inv_ref, share_ref, out_ref):
    devices = out_ref.shape[0]
    walk_dev, all_rows, _ = walk_ref.shape
    rows = all_rows // devices
    base = 2 * walk_dev * rows
    for w in range(walk_dev):
        inv = inv_ref[w]
        zero = jnp.zeros_like(inv)
        both = jnp.concatenate(
            [jnp.concatenate([inv, zero], 1), jnp.concatenate([zero, inv], 1)], 0
        )
        coefficients = walk_ref[w]
        greens = lax.dot_general(
            coefficients, both, (((1,), (1,)), ((), ())), preferred_element_type=F32
        ).astype(BF)
        for d in range(devices):
            piece = slice(d * rows, (d + 1) * rows)
            out_ref[d, w * rows : (w + 1) * rows, :] = greens[piece]
            at = (walk_dev + w) * rows
            out_ref[d, at : at + rows, :] = coefficients[piece]
    row = lax.broadcasted_iota(jnp.int32, (SLOT_ROWS, LANES), 0)
    lane = lax.broadcasted_iota(jnp.int32, (SLOT_ROWS, LANES), 1)
    tail = jnp.zeros((SLOT_ROWS, LANES), F32)
    for w in range(walk_dev):
        slot = slot_ref[w]
        low = jnp.broadcast_to(slot % RADIX, tail.shape).astype(F32)
        high = jnp.broadcast_to(slot // RADIX, tail.shape).astype(F32)
        here = lane == w
        tail = jnp.where(here & (row == 0), low, tail)
        tail = jnp.where(here & (row == 1), high, tail)
    for d in range(devices):
        out_ref[d, base : base + SLOT_ROWS, :] = tail.astype(BF)
        out_ref[d, base + SLOT_ROWS :, :] = share_ref[d]


def sort_kernel(core_ref, got_ref, green_ref, moved_ref, spread, seats, seat_smem, sem):
    devices, width, _ = got_ref.shape
    total, contract = green_ref.shape
    walk_dev = total // devices
    rows = contract // LANES
    base = 2 * walk_dev * rows
    share_rows = width - base - SLOT_ROWS
    each = share_rows // walk_dev
    core = core_ref[0]
    for d in range(devices):
        seats[d : d + 1, :] = (
            got_ref[d, base : base + 1, :].astype(F32)
            + RADIX * got_ref[d, base + 1 : base + 2, :].astype(F32)
        ).astype(jnp.int32)
    copy = pltpu.make_async_copy(seats, seat_smem, sem)
    copy.start()
    copy.wait()
    for d in range(devices):
        for w in range(walk_dev):
            slot = seat_smem[d, w]
            owner = slot // walk_dev
            side = jnp.where(owner % 2 == core, total // 2, 0)
            seat = side + (owner // 2) * walk_dev + w
            spread[pl.ds(seat, rows, stride=total), :] = got_ref[
                d, w * rows : (w + 1) * rows, :
            ].astype(F32)
            at = (walk_dev + w) * rows
            moved_ref[owner, w * rows : (w + 1) * rows, :] = got_ref[d, at : at + rows, :]
            tail = walk_dev * rows + w * each
            at = base + SLOT_ROWS + w * each
            moved_ref[owner, tail : tail + each, :] = got_ref[d, at : at + each, :]
    for r in range(rows):
        green_ref[:, r * LANES : (r + 1) * LANES] = spread[
            r * total : (r + 1) * total, :
        ].astype(BF)


def bias_kernel(green_ref, chol_ref, send_ref, keep_ref, buf, sem):
    slots, step, _ = buf.shape
    half = send_ref.shape[0]
    count = chol_ref.shape[0] // step

    def copy(i):
        return pltpu.make_async_copy(
            chol_ref.at[pl.ds(i * step, step)], buf.at[i % slots], sem.at[i % slots]
        )

    for i in range(min(slots, count)):
        copy(i).start()
    for i in range(count):
        copy(i).wait()
        part = jnp.dot(
            green_ref[:, i * step : (i + 1) * step],
            buf[i % slots],
            preferred_element_type=F32,
        )
        if i == 0:
            send_ref[...] = part[:half]
            keep_ref[...] = part[half:]
        else:
            send_ref[...] += part[:half]
            keep_ref[...] += part[half:]
        if i + slots < count:
            copy(i + slots).start()


def local(walkers, intersection_inv, new_slot, cholesky):
    devices = lax.axis_size("blk")
    me = lax.axis_index("blk")
    walk_dev = walkers.shape[0]
    total = walk_dev * devices
    occupied = cholesky.shape[1]
    contract = cholesky.shape[0] * occupied
    vectors = cholesky.shape[2]
    rows = contract // LANES
    chips = devices // 2
    chol = cholesky.reshape(contract, vectors)

    share = intersection_inv.shape[1] // devices
    share_pad = -share % LANES
    share_rows = walk_dev * (share + share_pad) // LANES
    width = 2 * walk_dev * rows + SLOT_ROWS + share_rows
    vmem = pl.BlockSpec(memory_space=pltpu.VMEM)
    smem = pl.BlockSpec(memory_space=pltpu.SMEM)
    hbm = pl.BlockSpec(memory_space=pl.ANY)

    packed = pl.pallas_call(
        greens_kernel,
        in_specs=[smem, vmem, vmem, vmem],
        out_specs=vmem,
        out_shape=jax.ShapeDtypeStruct((devices, width, LANES), BF),
    )(
        new_slot,
        walkers.reshape(walk_dev, devices * rows, LANES),
        intersection_inv.reshape(walk_dev, occupied, occupied),
        jnp.pad(
            intersection_inv.reshape(walk_dev, devices, share), ((0, 0), (0, 0), (0, share_pad))
        )
        .transpose(1, 0, 2)
        .reshape(devices, share_rows, LANES),
    )
    got = lax.all_to_all(packed, "blk", split_axis=0, concat_axis=0, tiled=True)

    greens, back = pl.pallas_call(
        sort_kernel,
        in_specs=[smem, vmem],
        out_specs=[vmem, vmem],
        out_shape=[
            jax.ShapeDtypeStruct((total, contract), BF),
            jax.ShapeDtypeStruct((devices, walk_dev * rows + share_rows, LANES), BF),
        ],
        scratch_shapes=[
            pltpu.VMEM((rows * total, LANES), F32),
            pltpu.VMEM((devices, LANES), jnp.int32),
            pltpu.SMEM((devices, LANES), jnp.int32),
            pltpu.SemaphoreType.DMA,
        ],
        compiler_params=pltpu.CompilerParams(vmem_limit_bytes=4 << 20),
    )((me % 2).reshape(1).astype(jnp.int32), got)

    moved = lax.all_to_all(back, "blk", split_axis=0, concat_axis=0, tiled=True)
    moved_walk = (
        moved[:, : walk_dev * rows]
        .reshape(devices, walk_dev, rows, LANES)
        .transpose(1, 0, 2, 3)
        .reshape(walk_dev, devices * contract)
    )
    moved_inverse = (
        moved[:, walk_dev * rows :]
        .reshape(devices, walk_dev, share + share_pad)[:, :, :share]
        .transpose(1, 0, 2)
        .reshape(walk_dev, devices * share)
    )

    half = total // 2
    step = min(LANES, contract // 4)
    ring = min(12, contract // step)
    bias_call = pl.pallas_call(
        bias_kernel,
        in_specs=[vmem, hbm],
        out_specs=[vmem, vmem],
        out_shape=[jax.ShapeDtypeStruct((half, vectors), F32)] * 2,
        scratch_shapes=[
            pltpu.VMEM((ring, step, vectors), BF),
            pltpu.SemaphoreType.DMA((ring,)),
        ],
        compiler_params=pltpu.CompilerParams(
            vmem_limit_bytes=ring * step * vectors * 2 + half * vectors * 8 + (4 << 20)
        ),
        cost_estimate=pl.CostEstimate(
            flops=60_000_000_000, bytes_accessed=contract * vectors * 2, transcendentals=0
        ),
    )
    send, keep = bias_call(greens, chol)

    pairs = [(i, i ^ 1) for i in range(devices)]
    both = keep + lax.ppermute(send, "blk", pairs)
    parts = both.astype(BF).reshape(chips, walk_dev, vectors)
    parity = [[2 * c + p for c in range(chips)] for p in range(2)]
    parts = lax.all_to_all(
        parts, "blk", split_axis=0, concat_axis=0, tiled=True, axis_index_groups=parity
    )
    bias = jnp.sum(parts.astype(F32), axis=0)
    return moved_walk, moved_inverse, bias


def solution(mesh):
    spec = P(("groups", "blk"), None)
    return jax.shard_map(
        local,
        mesh=mesh,
        in_specs=(spec, spec, P(("groups", "blk")), P(("groups", "blk"), None, None)),
        out_specs=(spec, spec, spec),
        check_vma=False,
    )
```

```python
import jax
import jax.numpy as jnp
from jax import lax
from jax.experimental import pallas as pl
from jax.experimental.pallas import tpu as pltpu
from jax.sharding import PartitionSpec as P


BF = jnp.bfloat16
F32 = jnp.float32
LANES = 128
SLOT_ROWS = 8
RADIX = 256
CORES = 2
DIRECT_CHIPS = 8


def target_chip(k, chips):
    if chips <= DIRECT_CHIPS:
        return lax.rem(lax.axis_index("blk") // CORES + k, chips)
    return k


def exchange(messages, chips):
    if chips > DIRECT_CHIPS:
        groups = [[CORES * c + p for c in range(chips)] for p in range(CORES)]
        got = lax.all_to_all(
            jnp.stack(messages),
            "blk",
            split_axis=0,
            concat_axis=0,
            tiled=True,
            axis_index_groups=groups,
        )
        return [got[k] for k in range(chips)]
    got = [messages[0]]
    for k in range(1, chips):
        pairs = [
            (i, (i // CORES + k) % chips * CORES + i % CORES) for i in range(chips * CORES)
        ]
        got.append(lax.ppermute(messages[k], "blk", pairs))
    return got


def pack_kernel(mine_ref, theirs_ref, *refs):
    *out_refs, inverse = refs
    chips = len(out_refs)
    devices = chips * CORES
    walk_dev, blocks, rows, _ = mine_ref.shape
    inv_rows = inverse.shape[0] // (CORES * walk_dev)
    inv_blocks = blocks - devices - 1
    per = LANES * inv_rows
    occupied = int(round(per**0.5))
    group = LANES // occupied
    share = -(-inv_rows // devices)
    walkers = CORES * walk_dev
    base = 2 * walkers * rows
    core = lax.rem(lax.axis_index("blk"), CORES)
    targets = [CORES * target_chip(k, chips) + core for k in range(chips)]
    new_row = lax.broadcasted_iota(jnp.int32, (occupied, occupied), 0)
    old_row = lax.broadcasted_iota(jnp.int32, (occupied, occupied), 1)
    order = (
        old_row == lax.rem(new_row, group) * (occupied // group) + lax.div(new_row, group)
    ).astype(BF)
    row = lax.broadcasted_iota(jnp.int32, (SLOT_ROWS, LANES), 0)
    lane = lax.broadcasted_iota(jnp.int32, (SLOT_ROWS, LANES), 1)
    tail = jnp.zeros((SLOT_ROWS, LANES), F32)
    for n in range(walkers):
        ref, w = (mine_ref, n) if n < walk_dev else (theirs_ref, n - walk_dev)
        flat = jnp.concatenate([ref[w, devices + b] for b in range(inv_blocks)], 0)
        inverse[n * inv_rows : (n + 1) * inv_rows, :] = flat.astype(F32)
        apart = jnp.concatenate(
            [flat[:, a * occupied : (a + 1) * occupied] for a in range(group)], 0
        )
        inv = jnp.dot(order, apart, preferred_element_type=F32).astype(BF)
        zero = jnp.zeros_like(inv)
        both = jnp.concatenate(
            [
                jnp.concatenate([inv if a == b else zero for b in range(group)], 1)
                for a in range(group)
            ],
            0,
        )
        coefficients = jnp.concatenate([ref[w, t] for t in targets], 0)
        greens = lax.dot_general(
            coefficients, both, (((1,), (1,)), ((), ())), preferred_element_type=F32
        ).astype(BF)
        for k in range(chips):
            piece = slice(k * rows, (k + 1) * rows)
            out_refs[k][n * rows : (n + 1) * rows, :] = greens[piece]
            at = (walkers + n) * rows
            out_refs[k][at : at + rows, :] = coefficients[piece]
        numbers = ref[w, blocks - 1].astype(F32)
        tail = jnp.where((lane == n) & (row == 0), numbers[0:1], tail)
        tail = jnp.where((lane == n) & (row == 1), numbers[1:2], tail)
    for k in range(chips):
        out_refs[k][base : base + SLOT_ROWS, :] = tail.astype(BF)
        first = jnp.minimum(targets[k] * share, inv_rows - share)
        for n in range(walkers):
            at = base + SLOT_ROWS + n * share
            out_refs[k][at : at + share, :] = inverse[
                pl.ds(n * inv_rows + first, share), :
            ].astype(BF)


def sort_kernel(*refs):
    *got_refs, green_ref, back_ref, spread, seats, seat_smem, sem = refs
    chips = len(got_refs)
    devices, back_rows, _ = back_ref.shape
    total, contract = green_ref.shape
    walk_dev = total // devices
    walkers = CORES * walk_dev
    rows = contract // LANES
    share = back_rows // walk_dev - rows
    base = 2 * walkers * rows
    core = lax.rem(lax.axis_index("blk"), CORES)
    for m in range(chips):
        low = got_refs[m][base : base + 1, :].astype(F32)
        high = got_refs[m][base + 1 : base + 2, :].astype(F32)
        seats[m : m + 1, :] = (low + RADIX * high).astype(jnp.int32)
    copy = pltpu.make_async_copy(seats, seat_smem, sem)
    copy.start()
    copy.wait()
    for m in range(chips):
        for n in range(walkers):
            w = n % walk_dev
            owner = lax.div(seat_smem[m, n], walk_dev)
            side = jnp.where(lax.rem(owner, CORES) == core, total // 2, 0)
            seat = side + lax.div(owner, CORES) * walk_dev + w
            spread[pl.ds(seat, rows, stride=total), :] = got_refs[m][
                n * rows : (n + 1) * rows, :
            ].astype(F32)
            at = (walkers + n) * rows
            back_ref[owner, w * rows : (w + 1) * rows, :] = got_refs[m][at : at + rows, :]
            tail = walk_dev * rows + w * share
            at = base + SLOT_ROWS + n * share
            back_ref[owner, tail : tail + share, :] = got_refs[m][at : at + share, :]
    for r in range(rows):
        green_ref[:, r * LANES : (r + 1) * LANES] = spread[
            r * total : (r + 1) * total, :
        ].astype(BF)


def prefetch_kernel(chol_ref, out_ref, sem):
    pieces = sem.shape[0]
    size = out_ref.shape[0] // pieces
    copies = [
        pltpu.make_async_copy(
            chol_ref.at[pl.ds(q * size, size)], out_ref.at[pl.ds(q * size, size)], sem.at[q]
        )
        for q in range(pieces)
    ]
    for copy in copies:
        copy.start()
    for copy in copies:
        copy.wait()


def bias_kernel(green_ref, early_ref, chol_ref, send_ref, keep_ref, buf, sem):
    early = early_ref.shape[0]
    slots, step, _ = buf.shape
    half = send_ref.shape[0]
    count = (chol_ref.shape[0] - early) // step

    def copy(i):
        return pltpu.make_async_copy(
            chol_ref.at[pl.ds(early + i * step, step)], buf.at[i % slots], sem.at[i % slots]
        )

    for i in range(min(slots, count)):
        copy(i).start()
    part = jnp.dot(green_ref[:, :early], early_ref[...], preferred_element_type=F32)
    send_ref[...] = part[:half]
    keep_ref[...] = part[half:]
    for i in range(count):
        copy(i).wait()
        part = jnp.dot(
            green_ref[:, early + i * step : early + (i + 1) * step],
            buf[i % slots],
            preferred_element_type=F32,
        )
        send_ref[...] += part[:half]
        keep_ref[...] += part[half:]
        if i + slots < count:
            copy(i + slots).start()


def fold_kernel(keep_ref, got_ref, *refs):
    *out_refs, spread = refs
    chips = len(out_refs)
    half, vectors = keep_ref.shape
    lines = vectors // LANES
    walk_dev = half // chips
    for j in range(lines):
        at = slice(j * LANES, (j + 1) * LANES)
        spread[pl.ds(j, half, stride=lines), :] = keep_ref[:, at] + got_ref[:, at]
    for k in range(chips):
        first = target_chip(k, chips) * (walk_dev * lines)
        if not isinstance(first, int):
            first = pl.multiple_of(first, 8)
        out_refs[k][...] = spread[pl.ds(first, walk_dev * lines), :].astype(BF)


def sum_kernel(*refs):
    *got_refs, out_ref, spread = refs
    total = got_refs[0][...].astype(F32)
    for ref in got_refs[1:]:
        total = total + ref[...].astype(F32)
    spread[...] = total
    walk_dev, vectors = out_ref.shape
    lines = vectors // LANES
    for j in range(lines):
        out_ref[:, j * LANES : (j + 1) * LANES] = spread[pl.ds(j, walk_dev, stride=lines), :]


def local(walkers, intersection_inv, new_slot, cholesky):
    devices = lax.axis_size("blk")
    chips = devices // CORES
    walk_dev = walkers.shape[0]
    total = walk_dev * devices
    half = total // 2
    contract = cholesky.shape[0] * cholesky.shape[1]
    vectors = cholesky.shape[2]
    rows = contract // LANES
    inv_rows = intersection_inv.shape[1] // LANES
    inv_blocks = -(-inv_rows // rows)
    blocks = devices + inv_blocks + 1
    share = -(-inv_rows // devices)
    chol = cholesky.reshape(contract, vectors)
    vmem = pl.BlockSpec(memory_space=pltpu.VMEM)
    hbm = pl.BlockSpec(memory_space=pl.ANY)

    def limit(size):
        return pltpu.CompilerParams(vmem_limit_bytes=size)

    place = lax.broadcasted_iota(jnp.int32, (walk_dev, rows * LANES), 1)
    slot = new_slot[:, None]
    number = jnp.where(place < LANES, slot % RADIX, slot // RADIX).astype(BF)
    mine = jnp.concatenate([walkers, intersection_inv, number], axis=1)
    mine = mine.reshape(walk_dev, blocks, rows, LANES)
    swap = [(i, i ^ 1) for i in range(devices)]
    theirs = lax.ppermute(mine, "blk", swap)

    width = 2 * CORES * walk_dev * rows + SLOT_ROWS + CORES * walk_dev * share
    messages = pl.pallas_call(
        pack_kernel,
        in_specs=[vmem, vmem],
        out_specs=[vmem] * chips,
        out_shape=[jax.ShapeDtypeStruct((width, LANES), BF)] * chips,
        scratch_shapes=[pltpu.VMEM((CORES * walk_dev * inv_rows, LANES), F32)],
        compiler_params=limit(8 << 20),
    )(mine, theirs)
    got = exchange(messages, chips)

    step = min(LANES, contract // 4)
    early = contract // 4 // step * step
    pieces = 8
    early_call = pl.pallas_call(
        prefetch_kernel,
        in_specs=[hbm],
        out_specs=vmem,
        out_shape=jax.ShapeDtypeStruct((early, vectors), BF),
        scratch_shapes=[pltpu.SemaphoreType.DMA((pieces,))],
        compiler_params=limit(2 << 20),
        cost_estimate=pl.CostEstimate(
            flops=8_000_000_000, bytes_accessed=early * vectors * 2, transcendentals=0
        ),
    )
    early_chol = early_call(chol)

    greens, back = pl.pallas_call(
        sort_kernel,
        in_specs=[vmem] * chips,
        out_specs=[vmem, vmem],
        out_shape=[
            jax.ShapeDtypeStruct((total, contract), BF),
            jax.ShapeDtypeStruct((devices, walk_dev * (rows + share), LANES), BF),
        ],
        scratch_shapes=[
            pltpu.VMEM((rows * total, LANES), F32),
            pltpu.VMEM((chips, LANES), jnp.int32),
            pltpu.SMEM((chips, LANES), jnp.int32),
            pltpu.SemaphoreType.DMA,
        ],
        compiler_params=limit(8 << 20),
    )(*got)

    ring = min(8, (contract - early) // step)
    send, keep = pl.pallas_call(
        bias_kernel,
        in_specs=[vmem, vmem, hbm],
        out_specs=[vmem, vmem],
        out_shape=[jax.ShapeDtypeStruct((half, vectors), F32)] * 2,
        scratch_shapes=[
            pltpu.VMEM((ring, step, vectors), BF),
            pltpu.SemaphoreType.DMA((ring,)),
        ],
        compiler_params=limit(ring * step * vectors * 2 + half * vectors * 8 + (4 << 20)),
        cost_estimate=pl.CostEstimate(
            flops=20_000_000_000, bytes_accessed=(contract - early) * vectors * 2, transcendentals=0
        ),
    )(greens, early_chol, chol)
    send, keep, back = lax.optimization_barrier((send, keep, back))

    moved = lax.all_to_all(back, "blk", split_axis=0, concat_axis=0, tiled=True)
    moved_walk = (
        moved[:, : walk_dev * rows]
        .reshape(devices, walk_dev, rows, LANES)
        .transpose(1, 0, 2, 3)
        .reshape(walkers.shape)
    )
    moved_inverse = (
        moved[:, walk_dev * rows :]
        .reshape(devices, walk_dev, share * LANES)
        .transpose(1, 0, 2)
        .reshape(walk_dev, devices * share * LANES)[:, : intersection_inv.shape[1]]
    )

    other = lax.ppermute(send, "blk", swap)
    lines = vectors // LANES
    fold_call = pl.pallas_call(
        fold_kernel,
        in_specs=[vmem, vmem],
        out_specs=[vmem] * chips,
        out_shape=[jax.ShapeDtypeStruct((walk_dev * lines, LANES), BF)] * chips,
        scratch_shapes=[pltpu.VMEM((half * lines, LANES), F32)],
        compiler_params=limit(half * vectors * 16 + (2 << 20)),
    )
    shares = fold_call(keep, other)
    shares = exchange(shares, chips)
    bias = pl.pallas_call(
        sum_kernel,
        in_specs=[vmem] * chips,
        out_specs=vmem,
        out_shape=jax.ShapeDtypeStruct((walk_dev, vectors), F32),
        scratch_shapes=[pltpu.VMEM((walk_dev * lines, LANES), F32)],
        compiler_params=limit(chips * walk_dev * vectors * 2 + (2 << 20)),
    )(*shares)
    return moved_walk, moved_inverse, bias


def solution(mesh):
    spec = P(("groups", "blk"), None)
    return jax.shard_map(
        local,
        mesh=mesh,
        in_specs=(spec, spec, P(("groups", "blk")), P(("groups", "blk"), None, None)),
        out_specs=(spec, spec, spec),
        check_vma=False,
    )
```

```python
import jax
import jax.numpy as jnp
from jax import lax
from jax.experimental import pallas as pl
from jax.experimental.pallas import tpu as pltpu
from jax.sharding import PartitionSpec as P


BF = jnp.bfloat16
F32 = jnp.float32
LANES = 128
SLOT_ROWS = 4
RADIX = 256
CORES = 2
DIRECT_CHIPS = 8
EARLY = 6


def paired(chips):
    return chips & (chips - 1) == 0


def apart(chip, k, chips):
    if isinstance(chip, int):
        return chip ^ k if paired(chips) else (chip + k) % chips
    return lax.bitwise_xor(chip, k) if paired(chips) else lax.rem(chip + k, chips)


def away(k, chips):
    return (chips - k) % chips


def my_core():
    return lax.rem(lax.axis_index("blk"), CORES)


def target_chip(k, chips):
    if chips > DIRECT_CHIPS:
        return k
    return apart(lax.div(lax.axis_index("blk"), CORES), away(k, chips), chips)


def source_chip(k, chips):
    if chips > DIRECT_CHIPS:
        return k
    k = away(k, chips)
    return apart(lax.div(lax.axis_index("blk"), CORES), k if paired(chips) else chips - k, chips)


def exchange(messages, chips):
    if chips > DIRECT_CHIPS:
        groups = [[CORES * c + p for c in range(chips)] for p in range(CORES)]
        got = lax.all_to_all(
            jnp.stack(messages),
            "blk",
            split_axis=0,
            concat_axis=0,
            tiled=True,
            axis_index_groups=groups,
        )
        return [got[k] for k in range(chips)]
    got = list(messages)
    for k in range(1, chips):
        pairs = [
            (i, apart(i // CORES, away(k, chips), chips) * CORES + i % CORES) for i in range(chips * CORES)
        ]
        got[k] = lax.ppermute(messages[k], "blk", pairs)
    return got


def fill_parts(slots, walk_ref, inv_ref, inverse, tile, parts):
    chips = len(parts)
    devices, block, _ = walk_ref.shape
    walk_dev = len(slots)
    inv_lines = inv_ref.shape[0]
    inv_rows = inv_lines // walk_dev
    occupied = int(round((LANES * inv_rows) ** 0.5))
    group = LANES // occupied
    share = -(-inv_rows // devices)
    lines = share * walk_dev
    core = my_core()
    targets = [CORES * target_chip(k, chips) + core for k in range(chips)]
    new_row = lax.broadcasted_iota(jnp.int32, (occupied, occupied), 0)
    old_row = lax.broadcasted_iota(jnp.int32, (occupied, occupied), 1)
    order = (
        old_row == lax.rem(new_row, group) * (occupied // group) + lax.div(new_row, group)
    ).astype(BF)
    line = lax.broadcasted_iota(jnp.int32, (chips * block, LANES), 0)
    tile[...] = jnp.zeros_like(tile)
    inverse[...] = inv_ref[...].astype(F32)
    coefficients = jnp.concatenate([walk_ref[t] for t in targets], 0)
    greens = None
    for w in range(walk_dev):
        flat = inverse[pl.ds(w, inv_rows, stride=walk_dev), :].astype(BF)
        split = jnp.concatenate(
            [flat[:, a * occupied : (a + 1) * occupied] for a in range(group)], 0
        )
        inv = jnp.dot(order, split, preferred_element_type=F32).astype(BF)
        zero = jnp.zeros_like(inv)
        both = jnp.concatenate(
            [
                jnp.concatenate([inv if a == b else zero for b in range(group)], 1)
                for a in range(group)
            ],
            0,
        )
        mine = lax.dot_general(
            coefficients, both, (((1,), (1,)), ((), ())), preferred_element_type=F32
        )
        greens = mine if w == 0 else jnp.where(lax.rem(line, walk_dev) == w, mine, greens)
        tile[0:1, w : w + 1] = lax.rem(slots[w], RADIX).astype(F32)
        tile[1:2, w : w + 1] = lax.div(slots[w], RADIX).astype(F32)
    greens = greens.astype(BF)
    for k, put in enumerate(parts):
        piece = slice(k * block, (k + 1) * block)
        put(0, greens[piece])
        put(block, coefficients[piece])
        first = jnp.minimum(targets[k] * share, inv_rows - share) * walk_dev
        put(2 * block, inverse[pl.ds(first, lines), :].astype(BF))
        put(2 * block + lines, tile[...].astype(BF))


def putter(ref, *index, start=0):
    def put(at, value):
        ref[(*index, slice(start + at, start + at + value.shape[0]), slice(None))] = value

    return put


def own_kernel(
    slot_hbm, walk_hbm, inv_hbm, out_ref, slot_ref, walk_ref, inv_ref, inverse, tile, sem
):
    copies = [
        pltpu.make_async_copy(source, target, sem.at[i])
        for i, (source, target) in enumerate(
            ((walk_hbm, walk_ref), (inv_hbm, inv_ref), (slot_hbm, slot_ref))
        )
    ]
    for copy in copies:
        copy.start()
    for copy in copies:
        copy.wait()
    slots = [jnp.full((1, 1), slot_ref[w], jnp.int32) for w in range(slot_ref.shape[0])]
    parts = [putter(out_ref, k) for k in range(out_ref.shape[0])]
    fill_parts(slots, walk_ref, inv_ref, inverse, tile, parts)


def pack_kernel(own_ref, slot_ref, walk_ref, inv_ref, *refs):
    *out_refs, inverse, tile = refs
    size = own_ref.shape[1]
    for k, ref in enumerate(out_refs):
        ref[:size, :] = own_ref[k]
    slots = [slot_ref[0:1, w : w + 1] for w in range(slot_ref.shape[1])]
    parts = [putter(ref, start=size) for ref in out_refs]
    fill_parts(slots, walk_ref, inv_ref, inverse, tile, parts)


def prefetch_kernel(chol_ref, out_ref, sem):
    pieces = sem.shape[0]
    size = out_ref.shape[0] // pieces
    copies = [
        pltpu.make_async_copy(
            chol_ref.at[pl.ds(q * size, size)], out_ref.at[pl.ds(q * size, size)], sem.at[q]
        )
        for q in range(pieces)
    ]
    for copy in copies:
        copy.start()
    for copy in copies:
        copy.wait()


def bias_kernel(*refs):
    *got_refs, early_ref, chol_ref, send_ref, keep_ref, back_send, back_keep = refs[:-9]
    buf, sem, green, text, spread, back, seats, seat_smem, seat_sem = refs[-9:]
    chips = len(got_refs)
    total, contract = green.shape
    early = early_ref.shape[0]
    slots, step, _ = buf.shape
    half = total // 2
    walk_dev = half // chips
    rows = contract // LANES
    block = rows * walk_dev
    back_rows = back_send.shape[1]
    lines = back_rows - block
    size = got_refs[0].shape[0] // CORES
    base = 2 * block + lines
    count = (contract - early) // step

    def copy(i):
        return pltpu.make_async_copy(
            chol_ref.at[pl.ds(early + i * step, step)], buf.at[i % slots], sem.at[i % slots]
        )

    for i in range(min(slots, count)):
        copy(i).start()

    for m in range(chips):
        for n in range(CORES):
            at = n * size + base
            low = got_refs[m][at : at + 1, :].astype(F32)
            high = got_refs[m][at + 1 : at + 2, :].astype(F32)
            at = m * CORES + n
            seats[at : at + 1, :] = (low + RADIX * high).astype(jnp.int32)
    seat_copy = pltpu.make_async_copy(seats, seat_smem, seat_sem)
    seat_copy.start()
    seat_copy.wait()
    core = my_core()
    for m in range(chips):
        text[m] = got_refs[m][...].astype(F32)
        for n in range(CORES):
            for w in range(walk_dev):
                at = n * size + w
                owner = lax.div(seat_smem[m * CORES + n, w], walk_dev)
                side = jnp.where(lax.rem(owner, CORES) == core, 1, 0)
                chip = lax.div(owner, CORES)
                seat = (side * walk_dev + w) * chips + chip
                spread[pl.ds(seat, rows, stride=total), :] = text[
                    m, pl.ds(at, rows, stride=walk_dev), :
                ]
                first = (side * chips + chip) * back_rows + w
                back[pl.ds(first, rows, stride=walk_dev), :] = text[
                    m, pl.ds(at + block, rows, stride=walk_dev), :
                ]
                for q in range(0, lines, walk_dev):
                    line = at + 2 * block + q
                    back[pl.ds(first + block + q, 1), :] = text[m, line : line + 1, :]
    for r in range(rows):
        green[:, r * LANES : (r + 1) * LANES] = spread[r * total : (r + 1) * total, :].astype(BF)
    for c in range(chips):
        back_send[c] = back[c * back_rows : (c + 1) * back_rows, :].astype(BF)
        at = (chips + c) * back_rows
        back_keep[c] = back[at : at + back_rows, :].astype(BF)

    part = jnp.dot(green[:, :early], early_ref[...], preferred_element_type=F32)
    send_ref[...] = part[:half]
    keep_ref[...] = part[half:]
    for i in range(count):
        copy(i).wait()
        part = jnp.dot(
            green[:, early + i * step : early + (i + 1) * step],
            buf[i % slots],
            preferred_element_type=F32,
        )
        send_ref[...] += part[:half]
        keep_ref[...] += part[half:]
        if i + slots < count:
            copy(i + slots).start()


def fold_kernel(keep_ref, got_ref, back_keep, back_got, *refs):
    *out_refs, spread = refs
    chips = len(out_refs)
    half, vectors = keep_ref.shape
    walk_dev = half // chips
    size = vectors // LANES * walk_dev
    back_rows = back_keep.shape[1]
    for j in range(vectors // LANES):
        at = slice(j * LANES, (j + 1) * LANES)
        both = keep_ref[:, at] + got_ref[:, at]
        for w in range(walk_dev):
            spread[pl.ds(j * walk_dev + w, chips, stride=size), :] = both[
                w * chips : (w + 1) * chips
            ]
    for k in range(chips):
        chip = target_chip(k, chips)
        first = chip * size
        if not isinstance(first, int):
            first = pl.multiple_of(first, 8)
        out_refs[k][:size, :] = spread[pl.ds(first, size), :].astype(BF)
        out_refs[k][size : size + back_rows, :] = back_keep[chip]
        out_refs[k][size + back_rows :, :] = back_got[chip]


def last_kernel(*refs):
    *got_refs, bias_ref, walk_ref, inv_ref, inverse = refs
    chips = len(got_refs)
    devices, block, _ = walk_ref.shape
    size = bias_ref.shape[0]
    lines = inverse.shape[0] // devices
    total = got_refs[0][:size, :].astype(F32)
    for ref in got_refs[1:]:
        total = total + ref[:size, :].astype(F32)
    bias_ref[...] = total
    core = my_core()
    for k in range(chips):
        chip = CORES * source_chip(k, chips)
        for n, device in enumerate((chip + core, chip + 1 - core)):
            at = size + n * (block + lines)
            walk_ref[device] = got_refs[k][at : at + block, :]
            inverse[pl.ds(device * lines, lines), :] = got_refs[k][
                at + block : at + block + lines, :
            ].astype(F32)
    inv_ref[...] = inverse[: inv_ref.shape[0], :].astype(BF)


def lines_of(x):
    count, size = x.shape
    x = x.reshape(count, size // LANES, LANES).transpose(1, 0, 2)
    return x.reshape(count * size // LANES, LANES)


def walkers_of(x, count):
    return x.reshape(-1, count, LANES).transpose(1, 0, 2).reshape(count, -1)


def local(walkers, intersection_inv, new_slot, cholesky):
    devices = lax.axis_size("blk")
    chips = devices // CORES
    walk_dev = walkers.shape[0]
    total = walk_dev * devices
    half = total // 2
    contract = cholesky.shape[0] * cholesky.shape[1]
    vectors = cholesky.shape[2]
    rows = contract // LANES
    block = rows * walk_dev
    inv_rows = intersection_inv.shape[1] // LANES
    lines = -(-inv_rows // devices) * walk_dev
    chol = cholesky.reshape(contract, vectors)
    vmem = pl.BlockSpec(memory_space=pltpu.VMEM)
    far = pl.BlockSpec(memory_space=pltpu.HBM)
    hbm = pl.BlockSpec(memory_space=pl.ANY)

    def limit(size):
        return pltpu.CompilerParams(vmem_limit_bytes=size)

    def out(*shape, dtype=BF):
        return jax.ShapeDtypeStruct(shape, dtype)

    swap = [(i, i ^ 1) for i in range(devices)]

    part = 2 * block + lines + SLOT_ROWS
    width = CORES * part
    walk = lines_of(walkers).reshape(devices, block, LANES)
    inverse = lines_of(intersection_inv)
    own_call = pl.pallas_call(
        own_kernel,
        in_specs=[far, far, far],
        out_specs=vmem,
        out_shape=pltpu.VMEM((chips, part, LANES), BF),
        scratch_shapes=[
            pltpu.SMEM(new_slot.shape, jnp.int32),
            pltpu.VMEM(walk.shape, BF),
            pltpu.VMEM(inverse.shape, BF),
            pltpu.VMEM(inverse.shape, F32),
            pltpu.VMEM((SLOT_ROWS, LANES), F32),
            pltpu.SemaphoreType.DMA((3,)),
        ],
        compiler_params=limit(8 << 20),
        cost_estimate=pl.CostEstimate(flops=500_000_000, bytes_accessed=0, transcendentals=0),
    )
    their_walk = lax.ppermute(walk, "blk", swap)
    their_inverse = lax.ppermute(inverse, "blk", swap)
    their_slot = lax.ppermute(new_slot.reshape(1, walk_dev), "blk", swap)
    own = own_call(
        *(
            pltpu.with_memory_space_constraint(x, pltpu.HBM)
            for x in (new_slot, walk, inverse)
        )
    )
    messages = pl.pallas_call(
        pack_kernel,
        in_specs=[vmem] * 4,
        out_specs=[vmem] * chips,
        out_shape=[out(width, LANES)] * chips,
        scratch_shapes=[pltpu.VMEM(inverse.shape, F32), pltpu.VMEM((SLOT_ROWS, LANES), F32)],
        compiler_params=limit(8 << 20),
    )(own, their_slot, their_walk, their_inverse)
    got = exchange(messages, chips)

    step = min(LANES, contract // 4)
    early = max(step, contract * EARLY // 32 // step * step)
    pieces = 8
    early_call = pl.pallas_call(
        prefetch_kernel,
        in_specs=[hbm],
        out_specs=vmem,
        out_shape=out(early, vectors),
        scratch_shapes=[pltpu.SemaphoreType.DMA((pieces,))],
        compiler_params=limit(2 << 20),
        cost_estimate=pl.CostEstimate(
            flops=8_000_000_000, bytes_accessed=early * vectors * 2, transcendentals=0
        ),
    )
    early_chol = early_call(chol)

    ring = min(8, (contract - early) // step)
    back_rows = block + lines
    send, keep, back_send, back_keep = pl.pallas_call(
        bias_kernel,
        in_specs=[vmem] * (chips + 1) + [hbm],
        out_specs=[vmem] * 4,
        out_shape=[out(half, vectors, dtype=F32)] * 2 + [out(chips, back_rows, LANES)] * 2,
        scratch_shapes=[
            pltpu.VMEM((ring, step, vectors), BF),
            pltpu.SemaphoreType.DMA((ring,)),
            pltpu.VMEM((total, contract), BF),
            pltpu.VMEM((chips, width, LANES), F32),
            pltpu.VMEM((rows * total, LANES), F32),
            pltpu.VMEM((2 * chips * back_rows, LANES), F32),
            pltpu.VMEM((chips * CORES, LANES), jnp.int32),
            pltpu.SMEM((chips * CORES, LANES), jnp.int32),
            pltpu.SemaphoreType.DMA,
        ],
        compiler_params=limit(ring * step * vectors * 2 + half * vectors * 8 + (8 << 20)),
        cost_estimate=pl.CostEstimate(
            flops=20_000_000_000, bytes_accessed=(contract - early) * vectors * 2, transcendentals=0
        ),
    )(*got, early_chol, chol)

    other = lax.ppermute(send, "blk", swap)
    back_other = lax.ppermute(back_send, "blk", swap)
    size = vectors // LANES * walk_dev
    shares = pl.pallas_call(
        fold_kernel,
        in_specs=[vmem] * 4,
        out_specs=[vmem] * chips,
        out_shape=[out(size + CORES * back_rows, LANES)] * chips,
        scratch_shapes=[pltpu.VMEM((chips * size, LANES), F32)],
        compiler_params=limit(half * vectors * 16 + (4 << 20)),
    )(keep, other, back_keep, back_other)
    shares = exchange(shares, chips)
    bias, moved_walk, moved_inverse = pl.pallas_call(
        last_kernel,
        in_specs=[vmem] * chips,
        out_specs=[vmem] * 3,
        out_shape=[
            out(size, LANES, dtype=F32),
            out(devices, block, LANES),
            out(inv_rows * walk_dev, LANES),
        ],
        scratch_shapes=[pltpu.VMEM((devices * lines, LANES), F32)],
        compiler_params=limit(chips * walk_dev * vectors * 4 + (4 << 20)),
    )(*shares)
    return (
        walkers_of(moved_walk.reshape(devices * block, LANES), walk_dev),
        walkers_of(moved_inverse, walk_dev),
        walkers_of(bias, walk_dev),
    )


def solution(mesh):
    spec = P(("groups", "blk"), None)
    return jax.shard_map(
        local,
        mesh=mesh,
        in_specs=(spec, spec, P(("groups", "blk")), P(("groups", "blk"), None, None)),
        out_specs=(spec, spec, spec),
        check_vma=False,
    )
```

```python
import functools

import jax
import jax.numpy as jnp
from jax import lax
from jax.experimental import pallas as pl
from jax.experimental.pallas import tpu as pltpu
from jax.sharding import PartitionSpec as P


BF = jnp.bfloat16
F32 = jnp.float32
LANES = 128
SLOT_ROWS = 4
RADIX = 256
CORES = 2
DIRECT_CHIPS = 8
EARLY = 8
MIRRORED = 12
SPARE = 8
ORDER = (0, 4, 2, 5, 6, 3, 7, 1)


def paired(chips):
    return chips & (chips - 1) == 0


def apart(chip, k, chips):
    if isinstance(chip, int):
        return chip ^ k if paired(chips) else (chip + k) % chips
    return lax.bitwise_xor(chip, k) if paired(chips) else lax.rem(chip + k, chips)


def away(k, chips):
    if chips == len(ORDER):
        return ORDER[k]
    half = chips // 2
    return [0, *range(half, chips), *range(half - 1, 0, -1)][k]


def mirror(chips):
    return chips // 2 if 4 <= chips <= DIRECT_CHIPS and paired(chips) else 0


def is_near(k, chips):
    return away(k, chips) < mirror(chips)


def my_core():
    return lax.rem(lax.axis_index("blk"), CORES)


def target_chip(k, chips):
    if chips > DIRECT_CHIPS:
        return k
    return apart(lax.div(lax.axis_index("blk"), CORES), away(k, chips), chips)


def source_chip(k, chips):
    if chips > DIRECT_CHIPS:
        return k
    k = away(k, chips)
    return apart(lax.div(lax.axis_index("blk"), CORES), k if paired(chips) else chips - k, chips)


def exchange(messages, chips):
    if chips > DIRECT_CHIPS:
        groups = [[CORES * c + p for c in range(chips)] for p in range(CORES)]
        got = lax.all_to_all(
            jnp.stack(messages),
            "blk",
            split_axis=0,
            concat_axis=0,
            tiled=True,
            axis_index_groups=groups,
        )
        return [got[k] for k in range(chips)]
    got = list(messages)
    for k in range(1, chips):
        pairs = [
            (i, apart(i // CORES, away(k, chips), chips) * CORES + i % CORES) for i in range(chips * CORES)
        ]
        got[k] = lax.ppermute(messages[k], "blk", pairs)
    return got


def fill_parts(extra, slots, walk_ref, inv_ref, inverse, tile, parts):
    chips = len(parts)
    devices, block, _ = walk_ref.shape
    walk_dev = len(slots)
    inv_lines = inv_ref.shape[0]
    inv_rows = inv_lines // walk_dev
    occupied = int(round((LANES * inv_rows) ** 0.5))
    group = LANES // occupied
    share = -(-inv_rows // devices)
    lines = share * walk_dev
    core = my_core()
    targets = [CORES * target_chip(k, chips) + core for k in range(chips)]
    new_row = lax.broadcasted_iota(jnp.int32, (occupied, occupied), 0)
    old_row = lax.broadcasted_iota(jnp.int32, (occupied, occupied), 1)
    order = (
        old_row == lax.rem(new_row, group) * (occupied // group) + lax.div(new_row, group)
    ).astype(BF)
    line = lax.broadcasted_iota(jnp.int32, (chips * block, LANES), 0)
    tile[...] = jnp.zeros_like(tile)
    inverse[:inv_lines, :] = inv_ref[...].astype(F32)
    coefficients = jnp.concatenate([walk_ref[t] for t in targets], 0)
    greens = None
    for w in range(walk_dev):
        flat = inverse[pl.ds(w, inv_rows, stride=walk_dev), :].astype(BF)
        split = jnp.concatenate(
            [flat[:, a * occupied : (a + 1) * occupied] for a in range(group)], 0
        )
        inv = jnp.dot(order, split, preferred_element_type=F32).astype(BF)
        zero = jnp.zeros_like(inv)
        both = jnp.concatenate(
            [
                jnp.concatenate([inv if a == b else zero for b in range(group)], 1)
                for a in range(group)
            ],
            0,
        )
        mine = lax.dot_general(
            coefficients, both, (((1,), (1,)), ((), ())), preferred_element_type=F32
        )
        greens = mine if w == 0 else jnp.where(lax.rem(line, walk_dev) == w, mine, greens)
        tile[0:1, w : w + 1] = lax.rem(slots[w], RADIX).astype(F32)
        tile[1:2, w : w + 1] = lax.div(slots[w], RADIX).astype(F32)
    greens = greens.astype(BF)
    for k, put in enumerate(parts):
        piece = slice(k * block, (k + 1) * block)
        put(0, greens[piece])
        put(block, coefficients[piece])
        first = jnp.minimum(targets[k] * share, inv_rows - share) * walk_dev
        if extra:
            across = CORES * lax.bitwise_xor(target_chip(k, chips), mirror(chips)) + core
            put(2 * block, walk_ref[across][:extra])
        put(2 * block + extra, inverse[pl.ds(first, lines), :].astype(BF))
        put(2 * block + extra + lines, tile[...].astype(BF))


def putter(ref, *index, start=0):
    def put(at, value):
        ref[(*index, slice(start + at, start + at + value.shape[0]), slice(None))] = value

    return put


def own_kernel(
    extra,
    slot_hbm,
    walk_hbm,
    inv_hbm,
    chol_hbm,
    out_ref,
    first_ref,
    slot_ref,
    walk_ref,
    inv_ref,
    inverse,
    tile,
    sem,
):
    first = pltpu.make_async_copy(
        chol_hbm.at[pl.ds(0, first_ref.shape[0])], first_ref, sem.at[3]
    )
    copies = [
        pltpu.make_async_copy(source, target, sem.at[i])
        for i, (source, target) in enumerate(
            ((walk_hbm, walk_ref), (inv_hbm, inv_ref), (slot_hbm, slot_ref))
        )
    ]
    for copy in copies:
        copy.start()
    first.start()
    for copy in copies:
        copy.wait()
    slots = [jnp.full((1, 1), slot_ref[w], jnp.int32) for w in range(slot_ref.shape[0])]
    parts = [putter(out_ref, k) for k in range(out_ref.shape[0])]
    fill_parts(extra, slots, walk_ref, inv_ref, inverse, tile, parts)
    first.wait()


def pack_kernel(extra, own_ref, slot_ref, walk_ref, inv_ref, *refs):
    *out_refs, inverse, tile = refs
    size = own_ref.shape[1]
    for k, ref in enumerate(out_refs):
        ref[:size, :] = own_ref[k]
    slots = [slot_ref[0:1, w : w + 1] for w in range(slot_ref.shape[1])]
    parts = [putter(ref, start=size) for ref in out_refs]
    fill_parts(extra, slots, walk_ref, inv_ref, inverse, tile, parts)


def prefetch_kernel(start, chol_ref, *refs):
    *out_refs, sem = refs
    pieces = sem.shape[0] // len(out_refs)
    copies = []
    for ref in out_refs:
        size = ref.shape[0] // pieces
        for q in range(pieces):
            copies.append(
                pltpu.make_async_copy(
                    chol_ref.at[pl.ds(start, size)],
                    ref.at[pl.ds(q * size, size)],
                    sem.at[len(copies)],
                )
            )
            start += size
    for copy in copies:
        copy.start()
    for copy in copies:
        copy.wait()


def bias_kernel(extra, chips, *refs):
    *in_refs, chol_ref, send_ref, keep_ref, back_send, back_keep = refs[:-9]
    got_refs, early_refs = in_refs[:chips], in_refs[chips:]
    buf, sem, green, text, spread, back, seats, seat_smem, seat_sem = refs[-9:]
    total, contract = green.shape
    early = sum(ref.shape[0] for ref in early_refs)
    slots, step, _ = buf.shape
    half = total // 2
    walk_dev = half // chips
    rows = contract // LANES
    block = rows * walk_dev
    back_rows = back_send.shape[1]
    lines = back_rows - block - extra
    size = got_refs[0].shape[0] // CORES
    base = 2 * block + extra + lines
    count = (contract - early) // step

    def copy(i):
        return pltpu.make_async_copy(
            chol_ref.at[pl.ds(early + i * step, step)], buf.at[i % slots], sem.at[i % slots]
        )

    for i in range(min(slots, count)):
        copy(i).start()

    for m in range(chips):
        for n in range(CORES):
            at = n * size + base
            low = got_refs[m][at : at + 1, :].astype(F32)
            high = got_refs[m][at + 1 : at + 2, :].astype(F32)
            at = m * CORES + n
            seats[at : at + 1, :] = (low + RADIX * high).astype(jnp.int32)
    seat_copy = pltpu.make_async_copy(seats, seat_smem, seat_sem)
    seat_copy.start()
    for m in range(chips):
        for n in range(CORES):
            text[m, n * size : n * size + block, :] = got_refs[m][
                n * size : n * size + block, :
            ].astype(F32)
    seat_copy.wait()
    core = my_core()

    def place(m, n, w):
        owner = lax.div(seat_smem[m * CORES + n, w], walk_dev)
        return jnp.where(lax.rem(owner, CORES) == core, 1, 0), lax.div(owner, CORES)

    for m in range(chips):
        for n in range(CORES):
            for w in range(walk_dev):
                side, chip = place(m, n, w)
                seat = (side * walk_dev + w) * chips + chip
                spread[pl.ds(seat, rows, stride=total), :] = text[
                    m, pl.ds(n * size + w, rows, stride=walk_dev), :
                ]
    for r in range(rows):
        green[:, r * LANES : (r + 1) * LANES] = spread[r * total : (r + 1) * total, :].astype(BF)

    def sort_back(m):
        for n in range(CORES):
            at = n * size + block
            text[m, at : at + base - block, :] = got_refs[m][at : at + base - block, :].astype(F32)
            for w in range(walk_dev):
                side, chip = place(m, n, w)
                first = (side * chips + chip) * back_rows + w
                count = (block + extra) // walk_dev
                back[pl.ds(first, count, stride=walk_dev), :] = text[
                    m, pl.ds(at + w, count, stride=walk_dev), :
                ]
                for q in range(block + extra, back_rows, walk_dev):
                    line = at + w + q
                    back[pl.ds(first + q, 1), :] = text[m, line : line + 1, :]

    part = None
    at = 0
    for ref in early_refs:
        mine = jnp.dot(green[:, at : at + ref.shape[0]], ref[...], preferred_element_type=F32)
        part = mine if part is None else part + mine
        at += ref.shape[0]
    send_ref[...] = part[:half]
    keep_ref[...] = part[half:]
    per = -(-chips // count)
    for i in range(count):
        copy(i).wait()
        part = jnp.dot(
            green[:, early + i * step : early + (i + 1) * step],
            buf[i % slots],
            preferred_element_type=F32,
        )
        send_ref[...] += part[:half]
        keep_ref[...] += part[half:]
        for m in range(i * per, min((i + 1) * per, chips)):
            sort_back(m)
        if i + slots < count:
            copy(i + slots).start()
    for c in range(chips):
        back_send[c] = back[c * back_rows : (c + 1) * back_rows, :].astype(BF)
        at = (chips + c) * back_rows
        back_keep[c] = back[at : at + back_rows, :].astype(BF)


def fold_kernel(extra, block, keep_ref, got_ref, back_keep, back_got, *refs):
    *out_refs, spread = refs
    chips = len(out_refs)
    half, vectors = keep_ref.shape
    walk_dev = half // chips
    size = vectors // LANES * walk_dev
    back_rows = back_keep.shape[1]
    for j in range(vectors // LANES):
        at = slice(j * LANES, (j + 1) * LANES)
        both = keep_ref[:, at] + got_ref[:, at]
        for w in range(walk_dev):
            spread[pl.ds(j * walk_dev + w, chips, stride=size), :] = both[
                w * chips : (w + 1) * chips
            ]
    for k in range(chips):
        chip = target_chip(k, chips)
        first = chip * size
        if not isinstance(first, int):
            first = pl.multiple_of(first, 8)
        out_refs[k][:size, :] = spread[pl.ds(first, size), :].astype(BF)
        if extra == 0 or is_near(k, chips):
            pieces = [slice(0, back_rows)]
        else:
            pieces = [slice(extra, block), slice(block + extra, back_rows)]
        at = size
        for ref in (back_keep, back_got):
            for piece in pieces:
                rows = piece.stop - piece.start
                out_refs[k][at : at + rows, :] = ref[chip][piece]
                at += rows


def last_kernel(extra, *refs):
    *got_refs, bias_ref, walk_ref, inv_ref, inverse = refs
    chips = len(got_refs)
    devices, block, _ = walk_ref.shape
    size = bias_ref.shape[0]
    lines = inverse.shape[0] // devices
    total = got_refs[0][:size, :].astype(F32)
    for ref in got_refs[1:]:
        total = total + ref[:size, :].astype(F32)
    bias_ref[...] = total
    core = my_core()
    for k in range(chips):
        chip = source_chip(k, chips)
        at = size
        for side in (core, 1 - core):
            device = CORES * chip + side
            if extra and not is_near(k, chips):
                walk_ref[device, extra:block, :] = got_refs[k][at : at + block - extra, :]
                at += block - extra
            else:
                walk_ref[device] = got_refs[k][at : at + block, :]
                at += block
                if extra:
                    across = CORES * lax.bitwise_xor(chip, mirror(chips)) + side
                    walk_ref[across, :extra, :] = got_refs[k][at : at + extra, :]
                    at += extra
            inverse[pl.ds(device * lines, lines), :] = got_refs[k][at : at + lines, :].astype(F32)
            at += lines
    inv_ref[...] = inverse[: inv_ref.shape[0], :].astype(BF)


def lines_of(x):
    count, size = x.shape
    x = x.reshape(count, size // LANES, LANES).transpose(1, 0, 2)
    return x.reshape(count * size // LANES, LANES)


def walkers_of(x, count):
    return x.reshape(-1, count, LANES).transpose(1, 0, 2).reshape(count, -1)


def local(walkers, intersection_inv, new_slot, cholesky):
    devices = lax.axis_size("blk")
    chips = devices // CORES
    walk_dev = walkers.shape[0]
    total = walk_dev * devices
    half = total // 2
    contract = cholesky.shape[0] * cholesky.shape[1]
    vectors = cholesky.shape[2]
    rows = contract // LANES
    block = rows * walk_dev
    inv_rows = intersection_inv.shape[1] // LANES
    lines = -(-inv_rows // devices) * walk_dev
    chol = cholesky.reshape(contract, vectors)
    vmem = pl.BlockSpec(memory_space=pltpu.VMEM)
    far = pl.BlockSpec(memory_space=pltpu.HBM)
    hbm = pl.BlockSpec(memory_space=pl.ANY)

    def limit(size):
        return pltpu.CompilerParams(vmem_limit_bytes=size)

    def out(*shape, dtype=BF):
        return jax.ShapeDtypeStruct(shape, dtype)

    swap = [(i, i ^ 1) for i in range(devices)]

    extra = rows * MIRRORED // 32 * walk_dev if mirror(chips) else 0
    part = 2 * block + extra + lines + SLOT_ROWS
    width = CORES * part
    walk = lines_of(walkers).reshape(devices, block, LANES)
    inverse = lines_of(intersection_inv)
    step = min(LANES, contract // 4)
    ahead = step
    own_call = pl.pallas_call(
        functools.partial(own_kernel, extra),
        in_specs=[far] * 4,
        out_specs=[vmem, vmem],
        out_shape=[pltpu.VMEM((chips, part, LANES), BF), pltpu.VMEM((ahead, vectors), BF)],
        scratch_shapes=[
            pltpu.SMEM(new_slot.shape, jnp.int32),
            pltpu.VMEM(walk.shape, BF),
            pltpu.VMEM(inverse.shape, BF),
            pltpu.VMEM((inverse.shape[0] + SPARE, LANES), F32),
            pltpu.VMEM((SLOT_ROWS, LANES), F32),
            pltpu.SemaphoreType.DMA((4,)),
        ],
        compiler_params=limit(8 << 20),
        cost_estimate=pl.CostEstimate(flops=500_000_000, bytes_accessed=0, transcendentals=0),
    )
    their_walk = lax.ppermute(walk, "blk", swap)
    their_inverse = lax.ppermute(inverse, "blk", swap)
    their_slot = lax.ppermute(new_slot.reshape(1, walk_dev), "blk", swap)
    own, first_chol = own_call(
        *(pltpu.with_memory_space_constraint(x, pltpu.HBM) for x in (new_slot, walk, inverse, chol))
    )
    messages = pl.pallas_call(
        functools.partial(pack_kernel, extra),
        in_specs=[vmem] * 4,
        out_specs=[vmem] * chips,
        out_shape=[out(width, LANES)] * chips,
        scratch_shapes=[pltpu.VMEM((inverse.shape[0] + SPARE, LANES), F32), pltpu.VMEM((SLOT_ROWS, LANES), F32)],
        compiler_params=limit(8 << 20),
    )(own, their_slot, their_walk, their_inverse)
    got = exchange(messages, chips)

    early = max(step, contract * EARLY // 32 // step * step)
    pieces = [early // 2 // step * step, early - early // 2 // step * step]
    pieces = [piece for piece in pieces if piece]
    early_call = pl.pallas_call(
        functools.partial(prefetch_kernel, ahead),
        in_specs=[hbm],
        out_specs=[vmem] * len(pieces),
        out_shape=[out(piece, vectors) for piece in pieces],
        scratch_shapes=[pltpu.SemaphoreType.DMA((4 * len(pieces),))],
        compiler_params=limit(2 << 20),
        cost_estimate=pl.CostEstimate(
            flops=8_000_000_000, bytes_accessed=early * vectors * 2, transcendentals=0
        ),
    )
    early_chol = early_call(chol)

    ring = max(2, min(8, contract * 17 // 32 // step - (ahead + early) // step))
    ring = min(ring, (contract - ahead - early) // step)
    back_rows = block + extra + lines
    send, keep, back_send, back_keep = pl.pallas_call(
        functools.partial(bias_kernel, extra, chips),
        in_specs=[vmem] * (chips + 1 + len(pieces)) + [hbm],
        out_specs=[vmem] * 4,
        out_shape=[out(half, vectors, dtype=F32)] * 2 + [out(chips, back_rows, LANES)] * 2,
        scratch_shapes=[
            pltpu.VMEM((ring, step, vectors), BF),
            pltpu.SemaphoreType.DMA((ring,)),
            pltpu.VMEM((total, contract), BF),
            pltpu.VMEM((chips, width + SPARE, LANES), F32),
            pltpu.VMEM((rows * total + total, LANES), F32),
            pltpu.VMEM((2 * chips * back_rows + SPARE, LANES), F32),
            pltpu.VMEM((chips * CORES, LANES), jnp.int32),
            pltpu.SMEM((chips * CORES, LANES), jnp.int32),
            pltpu.SemaphoreType.DMA,
        ],
        compiler_params=limit(
            ring * step * vectors * 2 + rows * total * LANES * 8 + (4 << 20)
            if chips <= DIRECT_CHIPS
            else 56 << 20
        ),
        cost_estimate=pl.CostEstimate(
            flops=20_000_000_000, bytes_accessed=(contract - early) * vectors * 2, transcendentals=0
        ),
    )(*got, first_chol, *early_chol, chol)

    other = lax.ppermute(send, "blk", swap)
    back_other = lax.ppermute(back_send, "blk", swap)
    size = vectors // LANES * walk_dev
    shares = pl.pallas_call(
        functools.partial(fold_kernel, extra, block),
        in_specs=[vmem] * 4,
        out_specs=[vmem] * chips,
        out_shape=[
            out(
                size + CORES * (block + lines + (extra if is_near(k, chips) else -extra)), LANES
            )
            for k in range(chips)
        ],
        scratch_shapes=[pltpu.VMEM((chips * size + size, LANES), F32)],
        compiler_params=limit(half * vectors * 16 + (4 << 20)),
    )(keep, other, back_keep, back_other)
    shares = exchange(shares, chips)
    bias, moved_walk, moved_inverse = pl.pallas_call(
        functools.partial(last_kernel, extra),
        in_specs=[vmem] * chips,
        out_specs=[vmem] * 3,
        out_shape=[
            out(size, LANES, dtype=F32),
            out(devices, block, LANES),
            out(inv_rows * walk_dev, LANES),
        ],
        scratch_shapes=[pltpu.VMEM((devices * lines, LANES), F32)],
        compiler_params=limit(chips * walk_dev * vectors * 4 + (4 << 20)),
    )(*shares)
    return (
        walkers_of(moved_walk.reshape(devices * block, LANES), walk_dev),
        walkers_of(moved_inverse, walk_dev),
        walkers_of(bias, walk_dev),
    )


def solution(mesh):
    spec = P(("groups", "blk"), None)
    return jax.shard_map(
        local,
        mesh=mesh,
        in_specs=(spec, spec, P(("groups", "blk")), P(("groups", "blk"), None, None)),
        out_specs=(spec, spec, spec),
        check_vma=False,
    )
```
